32 devices in a mesh: row: 4 (over x, core), col: 2 (over y), depth: 4 (over z).
Axes of the slice: x: 2, y: 2, z: 4, core: 2. Of those that a mesh axis runs over, the one named last changes fastest.
Arguments:
- tokens: bfloat16 [2048, 8192], P('col', ('row', 'depth')), may hold values from -6 to 6
- weight: bfloat16 [8192, 24576], P(('row', 'depth'), 'col'), may hold values from -0.0625 to 0.0625
- prev_tokens: bfloat16 [2048, 8192], P('col', ('row', 'depth')), may hold values from -6 to 6
- prev_grad: bfloat16 [2048, 24576], P(('row', 'depth'), 'col'), may hold values from -0.3125 to 0.3125
Outputs:
- qkv: bfloat16 [2048, 24576], P(('row', 'depth'), 'col')
- weight_grad: float32 [8192, 24576], P(('row', 'depth'), 'col')
The draws below stay inside these ranges and needn't reach their ends.
All inputs are finite; a program needn't handle non-finite values.
Results may differ from the reference program's by a relative error of at most 0.001.
Values may be sent and summed in bfloat16 or wider, within the bound.
A program may use at most 256 MiB of HBM per device.

```python
import jax
import jax.numpy as jnp

D = 8192
TOKENS = 2048


def raised(entries, rng, source, target, blocks, factor):
    owner, partner = [(jnp.arange(entries.shape[position]) // (entries.shape[position] // blocks)).reshape([-1 if axis == position else 1 for axis in range(entries.ndim)]) for position in (source, target)]
    chosen = jax.random.permutation(rng, blocks)[partner]
    strong = (owner == chosen) | (owner == (partner + blocks // 2) % blocks)
    return jnp.where(strong, factor * entries, entries)


def shard_levels(key, shape, split, low, high):
    level, own = 1.0, jax.random.fold_in(key, 6)
    for axis_at, shards_of in split:
        heights = jnp.exp(jax.random.uniform(jax.random.fold_in(own, axis_at), (shards_of,), jnp.float32, low / len(split), high / len(split)))
        level = level * jnp.repeat(heights, shape[axis_at] // shards_of).reshape([-1 if axis == axis_at else 1 for axis in range(len(shape))])
    return level


def bell_draw(key, dims, spread, bound, pieces=(), kind=jnp.bfloat16):
    gain = shard_levels(key, dims, pieces, -0.22, 0.18) if pieces else 1.0
    drawn = jax.random.normal(key, dims, jnp.float32) * spread * gain
    return jnp.minimum(jnp.maximum(drawn, -bound), bound).astype(kind)


def heavy_noise(key, shape, spread, most, split, heavy, held_as=jnp.bfloat16):
    entries = spread * jax.random.normal(key, shape, jnp.float32)
    if split:
        entries = entries * shard_levels(key, shape, split, -0.22, 0.18)
    return jnp.clip(raised(entries, jax.random.fold_in(key, 3), *heavy), -most, most).astype(held_as)


def setup_inputs(seed: int = 0) -> dict:
    arg_keys = jax.random.split(jax.random.key(seed), 5)
    return {
        "tokens": heavy_noise(arg_keys[0], (TOKENS, D), 1.0, 6.0, ((0, 2), (1, 16)), (1, 0, 16, 2.0)),
        "weight": bell_draw(arg_keys[1], (D, 3 * D), D ** -0.5, 0.0625, ((0, 16), (1, 2))),
        "prev_tokens": bell_draw(arg_keys[2], (TOKENS, D), 1.0, 6.0, ((0, 2), (1, 16))),
        "prev_grad": bell_draw(arg_keys[3], (TOKENS, 3 * D), 0.02, 0.3125, ((0, 16), (1, 2))),
    }


def reference(tokens, weight, prev_tokens, prev_grad):
    qkv = jnp.dot(tokens, weight, preferred_element_type=jnp.float32).astype(jnp.bfloat16)
    weight_grad = jnp.dot(prev_tokens.T, prev_grad, preferred_element_type=jnp.float32)
    return qkv, weight_grad
```

```python
import functools

import jax
import jax.numpy as jnp
from jax import lax
from jax.experimental import pallas as pl
from jax.experimental.pallas import tpu as pltpu
from jax.sharding import PartitionSpec as P

CC = 256
AHEAD = 8
RING = 8
PREFILL = 3
PIECES = 4
MESH = pl.DeviceIdType.MESH


def plain(tokens, weight, prev_tokens, prev_grad):
    rows_of_weight = lax.all_gather(weight, "row", axis=0, tiled=True)
    gathered = lax.all_gather(tokens, "col", axis=0, tiled=True)
    mine = lax.all_to_all(gathered, "row", split_axis=0, concat_axis=1, tiled=True)
    prev_gathered = lax.all_gather(prev_tokens, "col", axis=0, tiled=True)
    summed = lax.psum_scatter(
        jnp.dot(mine, rows_of_weight, preferred_element_type=jnp.float32),
        "depth",
        scatter_dimension=0,
        tiled=True,
    )
    weight_grad = lax.dot_general(
        prev_gathered,
        lax.all_gather(prev_grad, ("row", "depth"), axis=0, tiled=True),
        (((0,), (0,)), ((), ())),
        preferred_element_type=jnp.float32,
    )
    return (summed.astype(jnp.bfloat16), weight_grad)


def kernel(
    n, cols, carry,
    tokens, weight, grad,
    qkv, every, spread,
    tok, wslot, part, r1, r2, out,
    tok_local, tok_send, tok_recv, fan_send, fan_recv,
    w_send, w_recv, w_local,
    s1_send, s2_send, r1_recv, r2_recv,
    o_local, o_send, o_recv,
    g_send, g_recv, g_local, c_send, c_recv, x_send, x_recv, d_send, d_recv,
):
    row, col, z = lax.axis_index("row"), lax.axis_index("col"), lax.axis_index("depth")
    x, core = row // 2, row % 2
    half = n * CC
    own = grad.shape[0]
    piece = own // PIECES
    per_stage = PIECES + 1
    group = cols // 2
    local_rows = tokens.shape[0]
    in_half = lax.rem(col, group)
    holds = col // group == x
    end = (z == 0) | (z == 3)
    low = z < 2

    def flipped(m):
        a = core + (m % 2) - 2 * core * (m % 2)
        b = x + (m // 2) - 2 * x * (m // 2)
        return 2 * b + a

    near, over, cross = flipped(1), flipped(2), flipped(3)
    peers = {1: (near, col, z), 2: (over, col, z), 3: (cross, col, z)}

    def push(src, dst, ss, rs, to):
        return pltpu.make_async_remote_copy(src, dst, ss, rs, device_id=to, device_id_type=MESH)

    def w_copy(m, j):
        side = core if m == 2 else 1 - core
        at = pl.multiple_of(side * half + j * CC, CC)
        return push(weight.at[:, pl.ds(at, CC)], spread.at[j, m - 1], w_send.at[m - 1, j], w_recv.at[m - 1, j], peers[m])

    def w_loads(j):
        slot = lax.rem(j, 2)
        at = pl.multiple_of(core * half + j * CC, CC)
        rows = weight.shape[0]
        copies = [pltpu.make_async_copy(weight.at[:, pl.ds(at, CC)], wslot.at[slot, pl.ds(0, rows)], w_local.at[slot, 0])]
        for m in (1, 2, 3):
            copies.append(pltpu.make_async_copy(spread.at[j, m - 1], wslot.at[slot, pl.ds(m * rows, rows)], w_local.at[slot, m]))
        return copies

    def w_arrive(j):
        for m in (1, 2, 3):
            w_copy(m, j).wait_recv()
        for copy in w_loads(j):
            copy.start()

    def rows_of(r, d):
        return (r * 4 + d) * own

    def g_copy(way, s, q, to_next):
        step = 1 - 2 * way
        d = z - step * s
        to = (row, col, z + step) if to_next else (row, col, z)
        if q == PIECES:
            at = pl.ds(rows_of(over, d), carry)
            return push(every.at[at], every.at[at], g_send.at[way, s * per_stage + q], g_recv.at[way, s * per_stage + q], to)
        at = pl.ds(pl.multiple_of(rows_of(row, d) + q * piece, 16), piece)
        return push(every.at[at], every.at[at], g_send.at[way, s * per_stage + q], g_recv.at[way, s * per_stage + q], to)

    def g_own(way, q):
        step = 1 - 2 * way
        at = pl.ds(pl.multiple_of(rows_of(row, z) + q * piece, 16), piece)
        return push(grad.at[pl.ds(q * piece, piece)], every.at[at], g_send.at[way, q], g_recv.at[way, q], (row, col, z + step))

    def c_copy():
        return push(grad.at[pl.ds(0, carry)], every.at[pl.ds(rows_of(row, z), carry)], c_send.at[0], c_recv.at[0], peers[2])

    def c_landed():
        return push(grad.at[pl.ds(0, carry)], every.at[pl.ds(rows_of(over, z), carry)], c_send.at[0], c_recv.at[0], peers[2])

    def sends(way):
        return z < 3 if way == 0 else z > 0

    def has(way, s):
        return z >= s if way == 0 else z + s <= 3

    def g_recv_wait(way, s, q):
        step = 1 - 2 * way
        d = z - step * s
        if q == PIECES:
            at = pl.ds(rows_of(over, d), carry)
        else:
            at = pl.ds(pl.multiple_of(rows_of(row, d) + q * piece, 16), piece)
        index = (s - 1) * per_stage + q
        push(every.at[at], every.at[at], g_send.at[way, index], g_recv.at[way, index], (row, col, z)).wait_recv()

    def g_step(s, q):
        for way in (0, 1):
            if isinstance(s, int) and s == 0:
                if q < PIECES:
                    @pl.when(sends(way))
                    def _():
                        g_own(way, q).start()
                else:
                    @pl.when(sends(way))
                    def _():
                        g_copy(way, 0, q, True).start()
            else:
                @pl.when(has(way, s))
                def _():
                    g_recv_wait(way, s, q)

                    @pl.when(sends(way))
                    def _():
                        g_copy(way, s, q, True).start()

    def x_copy(d, i):
        rows = own - carry
        at = pl.ds(pl.multiple_of(rows_of(row, d) + carry, 16), rows)
        return push(every.at[at], every.at[at], x_send.at[i], x_recv.at[i], peers[2])

    def x_wait(d, i):
        rows = own - carry
        at = pl.ds(pl.multiple_of(rows_of(over, d) + carry, 16), rows)
        push(every.at[at], every.at[at], x_send.at[i], x_recv.at[i], peers[2]).wait_recv()

    def d_copy(r, d, i):
        at = pl.ds(pl.multiple_of(rows_of(r, d), 16), own)
        return push(every.at[at], every.at[at], d_send.at[i], d_recv.at[i], peers[1])

    def block_done(d):
        x_copy(d, d).start()
        d_copy(row, d, d).start()

    def stage_done(s):
        for way in (0, 1):
            step = 1 - 2 * way

            @pl.when(has(way, s))
            def _():
                block_done(z - step * s)

    def o_copies(j):
        slot = lax.rem(j, 4)
        at = pl.multiple_of(core * half + j * CC, CC)
        here = pltpu.make_async_copy(out.at[slot, core], qkv.at[:, pl.ds(at, CC)], o_local.at[slot])
        there = push(out.at[slot, 1 - core], qkv.at[:, pl.ds(at, CC)], o_send.at[slot], o_recv.at[j], peers[1])
        return here, there

    def o_wait(j):
        here, there = o_copies(j)
        here.wait()
        there.wait_send()

    def o_landed(j):
        slot = lax.rem(j, 4)
        at = pl.multiple_of((1 - core) * half + j * CC, CC)
        push(out.at[slot, core], qkv.at[:, pl.ds(at, CC)], o_send.at[slot], o_recv.at[j], peers[1]).wait_recv()

    def finish(j, value):
        @pl.when(j >= 4)
        def _():
            o_wait(j - 4)
        out[lax.rem(j, 4)] = value.astype(out.dtype)
        here, there = o_copies(j)
        here.start()
        there.start()

    def at_rows(a, b, size):
        return pl.ds(pl.multiple_of(jnp.where(low, a, b), own), size)

    def s1(j):
        slot = lax.rem(j, RING)
        return push(part.at[slot, :, at_rows(own, 0, 3 * own)], r1.at[j], s1_send.at[slot], r1_recv.at[j],
                    (row, col, jnp.where(low, 1, 2)))

    def s2(j):
        slot = lax.rem(j, RING)
        return push(part.at[slot, :, at_rows(2 * own, 0, 2 * own)], r2.at[j], s1_send.at[slot], r2_recv.at[j],
                    (row, col, jnp.where(low, 2, 1)))

    def s3(j):
        slot = lax.rem(j, RING)
        return push(part.at[slot, :, at_rows(0, 3 * own, own)], r2.at[j, :, pl.ds(0, own)], s2_send.at[slot], r2_recv.at[j],
                    (row, col, jnp.where(low, 0, 3)))

    def sent(j):
        @pl.when(end)
        def _():
            s1(j).wait_send()

        @pl.when(jnp.logical_not(end))
        def _():
            s2(j).wait_send()
            s3(j).wait_send()

    own_copy = pltpu.make_async_copy(grad, every.at[pl.ds(pl.multiple_of(rows_of(row, z), 16), own)], g_local.at[0])
    own_copy.start()
    place = pl.ds(pl.multiple_of(in_half * local_rows, 8), local_rows)
    hop = push(tokens, tok.at[2, place], tok_send.at[0], tok_recv.at[0], peers[2])
    keep = pltpu.make_async_copy(tokens, tok.at[0, place], tok_local.at[0])

    @pl.when(jnp.logical_not(holds))
    def _():
        hop.start()

    def fan(i, m):
        to = (row, lax.rem(col + i, cols), z)
        src = tokens if m == 0 else tok.at[2, place]
        return push(src, tok.at[2 * m, place], fan_send.at[m, i], fan_recv.at[m, in_half], to)

    @pl.when(holds)
    def _():
        keep.start()

        @pl.loop(1, cols)
        def _(i):
            fan(i, 0).start()

    w_copy(1, 0).start()
    w_copy(2, 0).start()
    w_copy(3, 0).start()
    c_copy().start()
    for q in range(PREFILL):
        g_step(0, q)

    @pl.loop(1, min(AHEAD, n))
    def _(j):
        for m in (1, 2, 3):
            w_copy(m, j).start()

    @pl.when(holds)
    def _():
        hop.wait_recv()

        @pl.loop(1, cols)
        def _(i):
            fan(i, 1).start()
        keep.wait()

    @pl.loop(0, group)
    def _(i):
        other = pl.ds(pl.multiple_of(i * local_rows, 8), local_rows)

        @pl.when(jnp.logical_or(jnp.logical_not(holds), i != in_half))
        def _():
            for m in (0, 1):
                push(tokens, tok.at[2 * m, other], fan_send.at[m, 0], fan_recv.at[m, i], (row, col, z)).wait_recv()

    pairs = [push(tok.at[2 * m], tok.at[2 * m + 1], tok_send.at[1 + m], tok_recv.at[1 + m], peers[1]) for m in (0, 1)]
    for copy in pairs:
        copy.start()
    w_arrive(0)
    for copy in pairs:
        copy.wait_recv()

    depth = weight.shape[0]
    total = max(n + 4, 4 * per_stage - PREFILL)

    @pl.loop(0, total)
    def _(t):
        @pl.when(t < n)
        def _():
            @pl.when(t >= RING)
            def _():
                sent(t - RING)
            for copy in w_loads(t):
                copy.wait()
            slot, ws = lax.rem(t, RING), lax.rem(t, 2)

            @pl.loop(0, 2)
            def _(h):
                rows = pl.ds(pl.multiple_of(h * 4 * own, own), 4 * own)
                acc = jnp.dot(tok[0, rows], wslot[ws, pl.ds(0, depth)], preferred_element_type=jnp.float32)
                for m in (1, 2, 3):
                    acc += jnp.dot(tok[m, rows], wslot[ws, pl.ds(m * depth, depth)], preferred_element_type=jnp.float32)
                part[slot, h] = acc

            @pl.when(end)
            def _():
                s1(t).start()

            @pl.when(t + AHEAD < n)
            def _():
                for m in (1, 2, 3):
                    w_copy(m, t + AHEAD).start()

            @pl.when(t + 1 < n)
            def _():
                w_arrive(t + 1)

        @pl.when(jnp.logical_not(end) & (t >= 1) & (t - 1 < n))
        def _():
            j = t - 1
            slot = lax.rem(j, RING)
            s1(j).wait_recv()
            rows = at_rows(2 * own, 0, 2 * own)
            part[slot, :, rows] = part[slot, :, rows] + r1[j, :, at_rows(own, 0, 2 * own)]
            s2(j).start()

        @pl.when(jnp.logical_not(end) & (t >= 2) & (t - 2 < n))
        def _():
            j = t - 2
            slot = lax.rem(j, RING)
            s2(j).wait_recv()
            rows = at_rows(0, 3 * own, own)
            part[slot, :, rows] = part[slot, :, rows] + r2[j, :, at_rows(0, own, own)]
            s3(j).start()
            mine = part[slot, :, at_rows(own, 2 * own, own)]
            finish(j, mine + r1[j, :, at_rows(0, 2 * own, own)] + r2[j, :, at_rows(own, 0, own)])

        @pl.when(end & (t >= 4) & (t - 4 < n))
        def _():
            j = t - 4
            s3(j).wait_recv()
            finish(j, part[lax.rem(j, RING), :, at_rows(0, 3 * own, own)] + r2[j, :, pl.ds(0, own)])

        p = t + PREFILL
        for q in range(PIECES + 1):
            if q >= PREFILL:
                @pl.when(p == q)
                def _():
                    if q == PIECES:
                        c_landed().wait_recv()
                    g_step(0, q)
            for s in (1, 2, 3):
                @pl.when(p == s * per_stage + q)
                def _():
                    g_step(s, q)
                    if q == PIECES:
                        stage_done(s)

        @pl.when(t == 2)
        def _():
            own_copy.wait()
            block_done(z)

    for i in range(4):
        x_wait(i, i)
        d_copy(over, i, 4 + i).start()

    @pl.loop(max(0, n - RING), n)
    def _(j):
        sent(j)

    @pl.loop(max(0, n - 4), n)
    def _(j):
        o_wait(j)

    @pl.loop(0, n)
    def _(j):
        o_landed(j)
        for m in (1, 2, 3):
            w_copy(m, j).wait_send()

    for way in (0, 1):
        @pl.when(sends(way))
        def _():
            for q in range(PIECES):
                g_own(way, q).wait_send()
            g_copy(way, 0, PIECES, True).wait_send()
        for s in (1, 2, 3):
            @pl.when(has(way, s) & sends(way))
            def _():
                for q in range(PIECES + 1):
                    g_copy(way, s, q, True).wait_send()
    c_copy().wait_send()
    for i in range(4):
        x_copy(i, i).wait_send()
        d_copy(row, i, i).wait_send()
        d_copy(over, i, 4 + i).wait_send()
        d_copy(near, i, i).wait_recv()
        d_copy(cross, i, 4 + i).wait_recv()

    @pl.when(jnp.logical_not(holds))
    def _():
        hop.wait_send()

    @pl.when(holds)
    def _():
        @pl.loop(1, cols)
        def _(i):
            fan(i, 0).wait_send()
            fan(i, 1).wait_send()
    for copy in pairs:
        copy.wait_send()


def local(cols, tokens, weight, prev_tokens, prev_grad):
    depth, width = weight.shape
    half = width // 2
    n = half // CC
    own = prev_grad.shape[0]
    carry = own * 3 // 8
    dma = pltpu.SemaphoreType.DMA
    anywhere = pl.BlockSpec(memory_space=pl.ANY)
    qkv, every, _ = pl.pallas_call(
        functools.partial(kernel, n, cols, carry),
        out_shape=(
            jax.ShapeDtypeStruct((own, width), jnp.bfloat16),
            jax.ShapeDtypeStruct((16 * own, width), jnp.bfloat16),
            jax.ShapeDtypeStruct((n, 3, depth, CC), jnp.bfloat16),
        ),
        in_specs=[anywhere] * 3,
        out_specs=(anywhere,) * 3,
        scratch_shapes=[
            pltpu.VMEM((4, 8 * own, depth), jnp.bfloat16),
            pltpu.VMEM((2, 4 * depth, CC), jnp.bfloat16),
            pltpu.VMEM((RING, 2, 4 * own, CC), jnp.float32),
            pltpu.VMEM((n, 2, 3 * own, CC), jnp.float32),
            pltpu.VMEM((n, 2, 2 * own, CC), jnp.float32),
            pltpu.VMEM((4, 2, own, CC), jnp.bfloat16),
            dma((1,)), dma((3,)), dma((3,)), dma((2, cols)), dma((2, cols // 2)),
            dma((3, n)), dma((3, n)), dma((2, 4)),
            dma((RING,)), dma((RING,)), dma((n,)), dma((n,)),
            dma((4,)), dma((4,)), dma((n,)),
            dma((2, 4 * (PIECES + 1))), dma((2, 4 * (PIECES + 1))), dma((1,)), dma((1,)), dma((1,)), dma((4,)), dma((4,)), dma((8,)), dma((8,)),
        ],
        compiler_params=pltpu.CompilerParams(has_side_effects=True, vmem_limit_bytes=64 * 1024 * 1024 - 65536),
        name="exchange",
    )(tokens, weight, prev_grad)
    prev_gathered = lax.all_gather(prev_tokens, "col", axis=0, tiled=True)
    weight_grad = lax.dot_general(prev_gathered, every, (((0,), (0,)), ((), ())), preferred_element_type=jnp.float32)
    return (qkv, weight_grad)


def solution(mesh):
    placed = (
        P("col", ("row", "depth")),
        P(("row", "depth"), "col"),
        P("col", ("row", "depth")),
        P(("row", "depth"), "col"),
    )
    cols = mesh.shape["col"]
    fits = mesh.shape["row"] == 4 and mesh.shape["depth"] == 4 and cols % 2 == 0
    return jax.shard_map(
        functools.partial(local, cols) if fits else plain,
        mesh=mesh,
        in_specs=placed,
        out_specs=(P(("row", "depth"), "col"), P(("row", "depth"), "col")),
        check_vma=False,
    )
```

```python
import functools
import math

import jax
import jax.numpy as jnp
from jax import lax
from jax.experimental import pallas as pl
from jax.experimental.pallas import tpu as pltpu
from jax.sharding import PartitionSpec as P

CC = 256
AHEAD = 8
RING = 8
PREFILL = 3
PIECES = 4
LATE, GAP = 13, 3
MESH = pl.DeviceIdType.MESH


def plain(tokens, weight, prev_tokens, prev_grad):
    rows_of_weight = lax.all_gather(weight, "row", axis=0, tiled=True)
    gathered = lax.all_gather(tokens, "col", axis=0, tiled=True)
    mine = lax.all_to_all(gathered, "row", split_axis=0, concat_axis=1, tiled=True)
    prev_gathered = lax.all_gather(prev_tokens, "col", axis=0, tiled=True)
    summed = lax.psum_scatter(
        jnp.dot(mine, rows_of_weight, preferred_element_type=jnp.float32),
        "depth",
        scatter_dimension=0,
        tiled=True,
    )
    weight_grad = lax.dot_general(
        prev_gathered,
        lax.all_gather(prev_grad, ("row", "depth"), axis=0, tiled=True),
        (((0,), (0,)), ((), ())),
        preferred_element_type=jnp.float32,
    )
    return (summed.astype(jnp.bfloat16), weight_grad)


def kernel(
    n, cols, carry,
    tokens, weight, prev, grad,
    qkv, every, prev_all, spread,
    tok, wslot, part, r1, r2, out,
    tok_local, tok_send, tok_recv, fan_send, fan_recv,
    w_send, w_recv, w_local,
    s1_send, s2_send, r1_recv, r2_recv,
    o_local, o_send, o_recv,
    g_send, g_recv, g_local, c_send, c_recv, x_send, x_recv, d_send, d_recv,
    p_local, p_send, p_recv,
):
    row, col, z = lax.axis_index("row"), lax.axis_index("col"), lax.axis_index("depth")
    x, core = row // 2, row % 2
    half = n * CC
    own = grad.shape[0]
    piece = own // PIECES
    per_stage = PIECES + 1
    group = cols // 2
    local_rows = tokens.shape[0]
    in_half = lax.rem(col, group)
    holds = col // group == x
    end = (z == 0) | (z == 3)
    low = z < 2

    def flipped(m):
        a = core + (m % 2) - 2 * core * (m % 2)
        b = x + (m // 2) - 2 * x * (m // 2)
        return 2 * b + a

    near, over, cross = flipped(1), flipped(2), flipped(3)
    peers = {1: (near, col, z), 2: (over, col, z), 3: (cross, col, z)}

    def push(src, dst, ss, rs, to):
        return pltpu.make_async_remote_copy(src, dst, ss, rs, device_id=to, device_id_type=MESH)

    def w_copy(m, j):
        side = core if m == 2 else 1 - core
        at = pl.multiple_of(side * half + j * CC, CC)
        return push(weight.at[:, pl.ds(at, CC)], spread.at[j, m - 1], w_send.at[m - 1, j], w_recv.at[m - 1, j], peers[m])

    def w_loads(j):
        slot = lax.rem(j, 2)
        at = pl.multiple_of(core * half + j * CC, CC)
        rows = weight.shape[0]
        copies = [pltpu.make_async_copy(weight.at[:, pl.ds(at, CC)], wslot.at[slot, pl.ds(0, rows)], w_local.at[slot, 0])]
        for m in (1, 2, 3):
            copies.append(pltpu.make_async_copy(spread.at[j, m - 1], wslot.at[slot, pl.ds(m * rows, rows)], w_local.at[slot, m]))
        return copies

    def w_arrive(j):
        for m in (1, 2, 3):
            w_copy(m, j).wait_recv()
        for copy in w_loads(j):
            copy.start()

    def rows_of(r, d):
        return (r * 4 + d) * own

    def g_copy(way, s, q, to_next):
        step = 1 - 2 * way
        d = z - step * s
        to = (row, col, z + step) if to_next else (row, col, z)
        if q == PIECES:
            at = pl.ds(rows_of(over, d), carry)
            return push(every.at[at], every.at[at], g_send.at[way, s * per_stage + q], g_recv.at[way, s * per_stage + q], to)
        at = pl.ds(pl.multiple_of(rows_of(row, d) + q * piece, 16), piece)
        return push(every.at[at], every.at[at], g_send.at[way, s * per_stage + q], g_recv.at[way, s * per_stage + q], to)

    def g_own(way, q):
        step = 1 - 2 * way
        at = pl.ds(pl.multiple_of(rows_of(row, z) + q * piece, 16), piece)
        return push(grad.at[pl.ds(q * piece, piece)], every.at[at], g_send.at[way, q], g_recv.at[way, q], (row, col, z + step))

    def c_copy():
        return push(grad.at[pl.ds(0, carry)], every.at[pl.ds(rows_of(row, z), carry)], c_send.at[0], c_recv.at[0], peers[2])

    def c_landed():
        return push(grad.at[pl.ds(0, carry)], every.at[pl.ds(rows_of(over, z), carry)], c_send.at[0], c_recv.at[0], peers[2])

    def sends(way):
        return z < 3 if way == 0 else z > 0

    def has(way, s):
        return z >= s if way == 0 else z + s <= 3

    def g_recv_wait(way, s, q):
        step = 1 - 2 * way
        d = z - step * s
        if q == PIECES:
            at = pl.ds(rows_of(over, d), carry)
        else:
            at = pl.ds(pl.multiple_of(rows_of(row, d) + q * piece, 16), piece)
        index = (s - 1) * per_stage + q
        push(every.at[at], every.at[at], g_send.at[way, index], g_recv.at[way, index], (row, col, z)).wait_recv()

    def g_step(s, q):
        for way in (0, 1):
            if isinstance(s, int) and s == 0:
                if q < PIECES:
                    @pl.when(sends(way))
                    def _():
                        g_own(way, q).start()
                else:
                    @pl.when(sends(way))
                    def _():
                        g_copy(way, 0, q, True).start()
            else:
                @pl.when(has(way, s))
                def _():
                    g_recv_wait(way, s, q)

                    @pl.when(sends(way))
                    def _():
                        g_copy(way, s, q, True).start()

    def x_copy(d, i):
        rows = own - carry
        at = pl.ds(pl.multiple_of(rows_of(row, d) + carry, 16), rows)
        return push(every.at[at], every.at[at], x_send.at[i], x_recv.at[i], peers[2])

    def x_wait(d, i):
        rows = own - carry
        at = pl.ds(pl.multiple_of(rows_of(over, d) + carry, 16), rows)
        push(every.at[at], every.at[at], x_send.at[i], x_recv.at[i], peers[2]).wait_recv()

    def d_copy(r, d, i):
        at = pl.ds(pl.multiple_of(rows_of(r, d), 16), own)
        return push(every.at[at], every.at[at], d_send.at[i], d_recv.at[i], peers[1])

    def block_done(d):
        x_copy(d, d).start()
        d_copy(row, d, d).start()

    def stage_done(s):
        for way in (0, 1):
            step = 1 - 2 * way

            @pl.when(has(way, s))
            def _():
                block_done(z - step * s)

    def crossed(d):
        x_wait(d, d)
        d_copy(over, d, 4 + d).start()

    def crossed_stage(s):
        for way in (0, 1):
            step = 1 - 2 * way

            @pl.when(has(way, s))
            def _():
                crossed(z - step * s)

    def o_copies(j):
        slot = lax.rem(j, 4)
        at = pl.multiple_of(core * half + j * CC, CC)
        here = pltpu.make_async_copy(out.at[slot, core], qkv.at[:, pl.ds(at, CC)], o_local.at[slot])
        there = push(out.at[slot, 1 - core], qkv.at[:, pl.ds(at, CC)], o_send.at[slot], o_recv.at[j], peers[1])
        return here, there

    def o_wait(j):
        here, there = o_copies(j)
        here.wait()
        there.wait_send()

    def o_landed(j):
        slot = lax.rem(j, 4)
        at = pl.multiple_of((1 - core) * half + j * CC, CC)
        push(out.at[slot, core], qkv.at[:, pl.ds(at, CC)], o_send.at[slot], o_recv.at[j], peers[1]).wait_recv()

    def finish(j, value):
        @pl.when(j >= 4)
        def _():
            o_wait(j - 4)
        out[lax.rem(j, 4)] = value.astype(out.dtype)
        here, there = o_copies(j)
        here.start()
        there.start()

    def at_rows(a, b, size):
        return pl.ds(pl.multiple_of(jnp.where(low, a, b), own), size)

    def s1(j):
        slot = lax.rem(j, RING)
        return push(part.at[slot, :, at_rows(own, 0, 3 * own)], r1.at[j], s1_send.at[slot], r1_recv.at[j],
                    (row, col, jnp.where(low, 1, 2)))

    def s2(j):
        slot = lax.rem(j, RING)
        return push(part.at[slot, :, at_rows(2 * own, 0, 2 * own)], r2.at[j], s1_send.at[slot], r2_recv.at[j],
                    (row, col, jnp.where(low, 2, 1)))

    def s3(j):
        slot = lax.rem(j, RING)
        return push(part.at[slot, :, at_rows(0, 3 * own, own)], r2.at[j, :, pl.ds(0, own)], s2_send.at[slot], r2_recv.at[j],
                    (row, col, jnp.where(low, 0, 3)))

    def sent(j):
        @pl.when(end)
        def _():
            s1(j).wait_send()

        @pl.when(jnp.logical_not(end))
        def _():
            s2(j).wait_send()
            s3(j).wait_send()

    own_copy = pltpu.make_async_copy(grad, every.at[pl.ds(pl.multiple_of(rows_of(row, z), 16), own)], g_local.at[0])
    own_copy.start()
    place = pl.ds(pl.multiple_of(in_half * local_rows, 8), local_rows)
    hop = push(tokens, tok.at[2, place], tok_send.at[0], tok_recv.at[0], peers[2])
    keep = pltpu.make_async_copy(tokens, tok.at[0, place], tok_local.at[0])

    @pl.when(jnp.logical_not(holds))
    def _():
        hop.start()

    def fan(i, m):
        to = (row, lax.rem(col + i, cols), z)
        src = tokens if m == 0 else tok.at[2, place]
        return push(src, tok.at[2 * m, place], fan_send.at[m, i], fan_recv.at[m, in_half], to)

    @pl.when(holds)
    def _():
        keep.start()

        @pl.loop(1, cols)
        def _(i):
            fan(i, 0).start()

    w_copy(1, 0).start()
    w_copy(2, 0).start()
    w_copy(3, 0).start()
    c_copy().start()
    for q in range(min(PREFILL, PIECES)):
        g_step(0, q)

    @pl.loop(1, min(AHEAD, n))
    def _(j):
        for m in (1, 2, 3):
            w_copy(m, j).start()

    @pl.when(holds)
    def _():
        hop.wait_recv()

        @pl.loop(1, cols)
        def _(i):
            fan(i, 1).start()
        keep.wait()

    if PREFILL > PIECES:
        c_landed().wait_recv()
        g_step(0, PIECES)

    @pl.loop(0, group)
    def _(i):
        other = pl.ds(pl.multiple_of(i * local_rows, 8), local_rows)

        @pl.when(jnp.logical_or(jnp.logical_not(holds), i != in_half))
        def _():
            for m in (0, 1):
                push(tokens, tok.at[2 * m, other], fan_send.at[m, 0], fan_recv.at[m, i], (row, col, z)).wait_recv()

    def p_copy(i):
        to = (row, lax.rem(col + i, cols), z)
        at = pl.ds(pl.multiple_of(col * local_rows, 8), local_rows)
        return push(prev, prev_all.at[at], p_send.at[i], p_recv.at[col], to)

    p_keep = pltpu.make_async_copy(prev, prev_all.at[pl.ds(pl.multiple_of(col * local_rows, 8), local_rows)], p_local.at[0])
    p_keep.start()

    @pl.loop(1, cols)
    def _(i):
        p_copy(i).start()

    pairs = [push(tok.at[2 * m], tok.at[2 * m + 1], tok_send.at[1 + m], tok_recv.at[1 + m], peers[1]) for m in (0, 1)]
    for copy in pairs:
        copy.start()
    w_arrive(0)
    for copy in pairs:
        copy.wait_recv()

    depth = weight.shape[0]
    total = max(n + 4, 4 * per_stage - PREFILL, LATE + 2 * GAP + 1)

    @pl.loop(0, total)
    def _(t):
        @pl.when(t < n)
        def _():
            @pl.when(t >= RING)
            def _():
                sent(t - RING)
            for copy in w_loads(t):
                copy.wait()
            slot, ws = lax.rem(t, RING), lax.rem(t, 2)

            @pl.loop(0, 2)
            def _(h):
                rows = pl.ds(pl.multiple_of(h * 4 * own, own), 4 * own)
                acc = jnp.dot(tok[0, rows], wslot[ws, pl.ds(0, depth)], preferred_element_type=jnp.float32)
                for m in (1, 2, 3):
                    acc += jnp.dot(tok[m, rows], wslot[ws, pl.ds(m * depth, depth)], preferred_element_type=jnp.float32)
                part[slot, h] = acc

            @pl.when(end)
            def _():
                s1(t).start()

            @pl.when(t + AHEAD < n)
            def _():
                for m in (1, 2, 3):
                    w_copy(m, t + AHEAD).start()

            @pl.when(t + 1 < n)
            def _():
                w_arrive(t + 1)

        @pl.when(jnp.logical_not(end) & (t >= 1) & (t - 1 < n))
        def _():
            j = t - 1
            slot = lax.rem(j, RING)
            s1(j).wait_recv()
            rows = at_rows(2 * own, 0, 2 * own)
            part[slot, :, rows] = part[slot, :, rows] + r1[j, :, at_rows(own, 0, 2 * own)]
            s2(j).start()

        @pl.when(jnp.logical_not(end) & (t >= 2) & (t - 2 < n))
        def _():
            j = t - 2
            slot = lax.rem(j, RING)
            s2(j).wait_recv()
            rows = at_rows(0, 3 * own, own)
            part[slot, :, rows] = part[slot, :, rows] + r2[j, :, at_rows(0, own, own)]
            s3(j).start()
            mine = part[slot, :, at_rows(own, 2 * own, own)]
            finish(j, mine + r1[j, :, at_rows(0, 2 * own, own)] + r2[j, :, at_rows(own, 0, own)])

        @pl.when(end & (t >= 4) & (t - 4 < n))
        def _():
            j = t - 4
            s3(j).wait_recv()
            finish(j, part[lax.rem(j, RING), :, at_rows(0, 3 * own, own)] + r2[j, :, pl.ds(0, own)])

        p = t + PREFILL
        for q in range(PIECES + 1):
            if q >= PREFILL:
                @pl.when(p == q)
                def _():
                    if q == PIECES:
                        c_landed().wait_recv()
                    g_step(0, q)
            for s in (1, 2, 3):
                @pl.when(p == s * per_stage + q)
                def _():
                    g_step(s, q)
                    if q == PIECES:
                        stage_done(s)

        @pl.when(t == 2)
        def _():
            own_copy.wait()
            block_done(z)

        @pl.when(t == LATE)
        def _():
            crossed(z)
        for s in (1, 2):
            @pl.when(t == LATE + GAP * s)
            def _():
                crossed_stage(s)

    p_keep.wait()

    @pl.loop(1, cols)
    def _(i):
        source = lax.rem(col + i, cols)
        at = pl.ds(pl.multiple_of(source * local_rows, 8), local_rows)
        push(prev, prev_all.at[at], p_send.at[i], p_recv.at[source], (row, col, z)).wait_recv()
        p_copy(i).wait_send()

    crossed_stage(3)

    @pl.loop(max(0, n - RING), n)
    def _(j):
        sent(j)

    @pl.loop(max(0, n - 4), n)
    def _(j):
        o_wait(j)

    @pl.loop(0, n)
    def _(j):
        o_landed(j)
        for m in (1, 2, 3):
            w_copy(m, j).wait_send()

    for way in (0, 1):
        @pl.when(sends(way))
        def _():
            for q in range(PIECES):
                g_own(way, q).wait_send()
            g_copy(way, 0, PIECES, True).wait_send()
        for s in (1, 2, 3):
            @pl.when(has(way, s) & sends(way))
            def _():
                for q in range(PIECES + 1):
                    g_copy(way, s, q, True).wait_send()
    c_copy().wait_send()
    for i in range(4):
        x_copy(i, i).wait_send()
        d_copy(row, i, i).wait_send()
        d_copy(over, i, 4 + i).wait_send()
        d_copy(near, i, i).wait_recv()
        d_copy(cross, i, 4 + i).wait_recv()

    @pl.when(jnp.logical_not(holds))
    def _():
        hop.wait_send()

    @pl.when(holds)
    def _():
        @pl.loop(1, cols)
        def _(i):
            fan(i, 0).wait_send()
            fan(i, 1).wait_send()
    for copy in pairs:
        copy.wait_send()


def product(left, right, out):
    out[...] = lax.dot_general(left[...], right[...], (((0,), (0,)), ((), ())), preferred_element_type=jnp.float32)


def local(cols, tokens, weight, prev_tokens, prev_grad):
    depth, width = weight.shape
    half = width // 2
    n = half // CC
    own = prev_grad.shape[0]
    carry = own // 4
    dma = pltpu.SemaphoreType.DMA
    anywhere = pl.BlockSpec(memory_space=pl.ANY)
    qkv, every, prev_all, _ = pl.pallas_call(
        functools.partial(kernel, n, cols, carry),
        out_shape=(
            jax.ShapeDtypeStruct((own, width), jnp.bfloat16),
            jax.ShapeDtypeStruct((16 * own, width), jnp.bfloat16),
            jax.ShapeDtypeStruct((8 * own * 2, depth), jnp.bfloat16),
            jax.ShapeDtypeStruct((n, 3, depth, CC), jnp.bfloat16),
        ),
        in_specs=[anywhere] * 4,
        out_specs=(anywhere,) * 4,
        scratch_shapes=[
            pltpu.VMEM((4, 8 * own, depth), jnp.bfloat16),
            pltpu.VMEM((2, 4 * depth, CC), jnp.bfloat16),
            pltpu.VMEM((RING, 2, 4 * own, CC), jnp.float32),
            pltpu.VMEM((n, 2, 3 * own, CC), jnp.float32),
            pltpu.VMEM((n, 2, 2 * own, CC), jnp.float32),
            pltpu.VMEM((4, 2, own, CC), jnp.bfloat16),
            dma((1,)), dma((3,)), dma((3,)), dma((2, cols)), dma((2, cols // 2)),
            dma((3, n)), dma((3, n)), dma((2, 4)),
            dma((RING,)), dma((RING,)), dma((n,)), dma((n,)),
            dma((4,)), dma((4,)), dma((n,)),
            dma((2, 4 * (PIECES + 1))), dma((2, 4 * (PIECES + 1))), dma((1,)), dma((1,)), dma((1,)), dma((4,)), dma((4,)), dma((8,)), dma((8,)),
            dma((1,)), dma((cols,)), dma((cols,)),
        ],
        compiler_params=pltpu.CompilerParams(has_side_effects=True, vmem_limit_bytes=64 * 1024 * 1024 - 65536),
        name="exchange",
    )(tokens, weight, prev_tokens, prev_grad)
    tile = math.gcd(width, 1536)
    weight_grad = pl.pallas_call(
        product,
        out_shape=jax.ShapeDtypeStruct((depth, width), jnp.float32),
        grid=(width // tile,),
        in_specs=[pl.BlockSpec((16 * own, depth), lambda i: (0, 0)), pl.BlockSpec((16 * own, tile), lambda i: (0, i))],
        out_specs=pl.BlockSpec((depth, tile), lambda i: (0, i)),
        compiler_params=pltpu.CompilerParams(vmem_limit_bytes=32 * 1024 * 1024),
        name="product",
    )(prev_all, every)
    return (qkv, weight_grad)


def solution(mesh):
    placed = (
        P("col", ("row", "depth")),
        P(("row", "depth"), "col"),
        P("col", ("row", "depth")),
        P(("row", "depth"), "col"),
    )
    cols = mesh.shape["col"]
    fits = mesh.shape["row"] == 4 and mesh.shape["depth"] == 4 and cols % 2 == 0
    return jax.shard_map(
        functools.partial(local, cols) if fits else plain,
        mesh=mesh,
        in_specs=placed,
        out_specs=(P(("row", "depth"), "col"), P(("row", "depth"), "col")),
        check_vma=False,
    )
```

```python
import functools
import math

import jax
import jax.numpy as jnp
from jax import lax
from jax.experimental import pallas as pl
from jax.experimental.pallas import tpu as pltpu
from jax.sharding import PartitionSpec as P

CC = 256
AHEAD = 8
RING = 8
PREFILL = 5
STEPS = 10
SCALE = 256 * (STEPS + 0.5)
PIECES = 4
LATE, GAP = 20, 5
REST = 3
MESH = pl.DeviceIdType.MESH


def plain(tokens, weight, prev_tokens, prev_grad):
    rows_of_weight = lax.all_gather(weight, "row", axis=0, tiled=True)
    gathered = lax.all_gather(tokens, "col", axis=0, tiled=True)
    mine = lax.all_to_all(gathered, "row", split_axis=0, concat_axis=1, tiled=True)
    prev_gathered = lax.all_gather(prev_tokens, "col", axis=0, tiled=True)
    summed = lax.psum_scatter(
        jnp.dot(mine, rows_of_weight, preferred_element_type=jnp.float32),
        "depth",
        scatter_dimension=0,
        tiled=True,
    )
    weight_grad = lax.dot_general(
        prev_gathered,
        lax.all_gather(prev_grad, ("row", "depth"), axis=0, tiled=True),
        (((0,), (0,)), ((), ())),
        preferred_element_type=jnp.float32,
    )
    return (summed.astype(jnp.bfloat16), weight_grad)


def code(ref, value):
    head = value.astype(jnp.bfloat16)
    wide = head.astype(jnp.float32)
    steps = jnp.round((value - wide) * SCALE / jnp.where(wide == 0, 1.0, wide))
    steps = jnp.clip(steps, -STEPS, STEPS)
    half = CC // 2
    ref[:, pl.ds(0, CC)] = head
    ref[:, pl.ds(CC, half)] = ((2 * STEPS + 1) * steps[:, :half] + steps[:, half:]).astype(jnp.bfloat16)


def decode(coded):
    head = coded[..., :CC].astype(jnp.float32)
    both = coded[..., CC:].astype(jnp.float32)
    upper = jnp.round(both * (1 / (2 * STEPS + 1)))
    steps = jnp.concatenate([upper, both - (2 * STEPS + 1) * upper], -1)
    return head + head * steps * (1 / SCALE)


def kernel(
    n, cols, carry,
    tokens, weight, prev, grad,
    qkv, every, prev_all, spread,
    tok, wslot, part, first, second, r1, r2, r3, out,
    tok_local, tok_send, tok_recv, fan_send, fan_recv,
    w_send, w_recv, w_local,
    s1_send, s2_send, r1_recv, r2_recv, r3_recv,
    o_local, o_send, o_recv,
    g_send, g_recv, g_local, c_send, c_recv, x_send, x_recv, d_send, d_recv,
    p_local, p_send, p_recv,
):
    row, col, z = lax.axis_index("row"), lax.axis_index("col"), lax.axis_index("depth")
    x, core = row // 2, row % 2
    half = n * CC
    own = grad.shape[0]
    piece = own // PIECES
    per_stage = PIECES + 1
    group = cols // 2
    local_rows = tokens.shape[0]
    in_half = lax.rem(col, group)
    holds = col // group == x
    end = (z == 0) | (z == 3)
    low = z < 2

    def flipped(m):
        a = core + (m % 2) - 2 * core * (m % 2)
        b = x + (m // 2) - 2 * x * (m // 2)
        return 2 * b + a

    near, over, cross = flipped(1), flipped(2), flipped(3)
    peers = {1: (near, col, z), 2: (over, col, z), 3: (cross, col, z)}

    def push(src, dst, ss, rs, to):
        return pltpu.make_async_remote_copy(src, dst, ss, rs, device_id=to, device_id_type=MESH)

    def w_copy(m, j):
        side = core if m == 2 else 1 - core
        at = pl.multiple_of(side * half + j * CC, CC)
        return push(weight.at[:, pl.ds(at, CC)], spread.at[j, m - 1], w_send.at[m - 1, j], w_recv.at[m - 1, j], peers[m])

    def w_loads(j):
        slot = lax.rem(j, 2)
        at = pl.multiple_of(core * half + j * CC, CC)
        rows = weight.shape[0]
        copies = [pltpu.make_async_copy(weight.at[:, pl.ds(at, CC)], wslot.at[slot, pl.ds(0, rows)], w_local.at[slot, 0])]
        for m in (1, 2, 3):
            copies.append(pltpu.make_async_copy(spread.at[j, m - 1], wslot.at[slot, pl.ds(m * rows, rows)], w_local.at[slot, m]))
        return copies

    def w_arrive(j):
        for m in (1, 2, 3):
            w_copy(m, j).wait_recv()
        for copy in w_loads(j):
            copy.start()

    def rows_of(r, d):
        return (r * 4 + d) * own

    def g_copy(way, s, q, to_next):
        step = 1 - 2 * way
        d = z - step * s
        to = (row, col, z + step) if to_next else (row, col, z)
        if q == PIECES:
            at = pl.ds(rows_of(over, d), carry)
            return push(every.at[at], every.at[at], g_send.at[way, s * per_stage + q], g_recv.at[way, s * per_stage + q], to)
        at = pl.ds(pl.multiple_of(rows_of(row, d) + q * piece, 16), piece)
        return push(every.at[at], every.at[at], g_send.at[way, s * per_stage + q], g_recv.at[way, s * per_stage + q], to)

    def g_own(way, q):
        step = 1 - 2 * way
        at = pl.ds(pl.multiple_of(rows_of(row, z) + q * piece, 16), piece)
        return push(grad.at[pl.ds(q * piece, piece)], every.at[at], g_send.at[way, q], g_recv.at[way, q], (row, col, z + step))

    def c_copy():
        return push(grad.at[pl.ds(0, carry)], every.at[pl.ds(rows_of(row, z), carry)], c_send.at[0], c_recv.at[0], peers[2])

    def c_landed():
        return push(grad.at[pl.ds(0, carry)], every.at[pl.ds(rows_of(over, z), carry)], c_send.at[0], c_recv.at[0], peers[2])

    def sends(way):
        return z < 3 if way == 0 else z > 0

    def has(way, s):
        return z >= s if way == 0 else z + s <= 3

    def g_recv_wait(way, s, q):
        step = 1 - 2 * way
        d = z - step * s
        if q == PIECES:
            at = pl.ds(rows_of(over, d), carry)
        else:
            at = pl.ds(pl.multiple_of(rows_of(row, d) + q * piece, 16), piece)
        index = (s - 1) * per_stage + q
        push(every.at[at], every.at[at], g_send.at[way, index], g_recv.at[way, index], (row, col, z)).wait_recv()

    def g_step(s, q):
        for way in (0, 1):
            if isinstance(s, int) and s == 0:
                if q < PIECES:
                    @pl.when(sends(way))
                    def _():
                        g_own(way, q).start()
                else:
                    @pl.when(sends(way))
                    def _():
                        g_copy(way, 0, q, True).start()
            else:
                @pl.when(has(way, s))
                def _():
                    g_recv_wait(way, s, q)

                    @pl.when(sends(way))
                    def _():
                        g_copy(way, s, q, True).start()

    def x_copy(d, i):
        rows = own - carry
        at = pl.ds(pl.multiple_of(rows_of(row, d) + carry, 16), rows)
        return push(every.at[at], every.at[at], x_send.at[i], x_recv.at[i], peers[2])

    def x_wait(d, i):
        rows = own - carry
        at = pl.ds(pl.multiple_of(rows_of(over, d) + carry, 16), rows)
        push(every.at[at], every.at[at], x_send.at[i], x_recv.at[i], peers[2]).wait_recv()

    def d_copy(r, d, i):
        at = pl.ds(pl.multiple_of(rows_of(r, d), 16), own)
        return push(every.at[at], every.at[at], d_send.at[i], d_recv.at[i], peers[1])

    def block_done(d):
        x_copy(d, d).start()
        d_copy(row, d, d).start()

    def stage_done(s):
        for way in (0, 1):
            step = 1 - 2 * way

            @pl.when(has(way, s))
            def _():
                block_done(z - step * s)

    def crossed(d):
        x_wait(d, d)
        d_copy(over, d, 4 + d).start()

    def crossed_stage(s):
        for way in (0, 1):
            step = 1 - 2 * way

            @pl.when(has(way, s))
            def _():
                crossed(z - step * s)

    def o_copies(j):
        slot = lax.rem(j, 4)
        at = pl.multiple_of(core * half + j * CC, CC)
        here = pltpu.make_async_copy(out.at[slot, core], qkv.at[:, pl.ds(at, CC)], o_local.at[slot])
        there = push(out.at[slot, 1 - core], qkv.at[:, pl.ds(at, CC)], o_send.at[slot], o_recv.at[j], peers[1])
        return here, there

    def o_wait(j):
        here, there = o_copies(j)
        here.wait()
        there.wait_send()

    def o_landed(j):
        slot = lax.rem(j, 4)
        at = pl.multiple_of((1 - core) * half + j * CC, CC)
        push(out.at[slot, core], qkv.at[:, pl.ds(at, CC)], o_send.at[slot], o_recv.at[j], peers[1]).wait_recv()

    def finish(j, value):
        @pl.when(j >= 4)
        def _():
            o_wait(j - 4)
        out[lax.rem(j, 4)] = value.astype(out.dtype)
        here, there = o_copies(j)
        here.start()
        there.start()

    def at_rows(a, b, size):
        return pl.ds(pl.multiple_of(jnp.where(low, a, b), own), size)

    def s1(j):
        slot = lax.rem(j, RING)
        return push(first.at[slot], r1.at[j], s1_send.at[slot], r1_recv.at[j],
                    (row, col, jnp.where(low, 1, 2)))

    def s2(j):
        slot = lax.rem(j, RING)
        return push(second.at[slot], r2.at[j], s1_send.at[slot], r2_recv.at[j],
                    (row, col, jnp.where(low, 2, 1)))

    def s3(j):
        slot = lax.rem(j, RING)
        return push(part.at[slot, :, at_rows(0, 3 * own, own)], r3.at[j], s2_send.at[slot], r3_recv.at[j],
                    (row, col, jnp.where(low, 0, 3)))

    def sent(j):
        @pl.when(end)
        def _():
            s1(j).wait_send()

        @pl.when(jnp.logical_not(end))
        def _():
            s2(j).wait_send()
            s3(j).wait_send()

    own_copy = pltpu.make_async_copy(grad, every.at[pl.ds(pl.multiple_of(rows_of(row, z), 16), own)], g_local.at[0])
    own_copy.start()
    place = pl.ds(pl.multiple_of(in_half * local_rows, 8), local_rows)
    hop = push(tokens, tok.at[2, place], tok_send.at[0], tok_recv.at[0], peers[2])
    keep = pltpu.make_async_copy(tokens, tok.at[0, place], tok_local.at[0])

    @pl.when(jnp.logical_not(holds))
    def _():
        hop.start()

    def fan(i, m):
        to = (row, lax.rem(col + i, cols), z)
        src = tokens if m == 0 else tok.at[2, place]
        return push(src, tok.at[2 * m, place], fan_send.at[m, i], fan_recv.at[m, in_half], to)

    @pl.when(holds)
    def _():
        keep.start()

        @pl.loop(1, cols)
        def _(i):
            fan(i, 0).start()

    w_copy(1, 0).start()
    w_copy(2, 0).start()
    w_copy(3, 0).start()
    c_copy().start()
    for q in range(min(PREFILL, PIECES)):
        g_step(0, q)

    @pl.loop(1, min(AHEAD, n))
    def _(j):
        for m in (1, 2, 3):
            w_copy(m, j).start()

    @pl.when(holds)
    def _():
        hop.wait_recv()

        @pl.loop(1, cols)
        def _(i):
            fan(i, 1).start()
        keep.wait()

    if PREFILL > PIECES:
        c_landed().wait_recv()
        g_step(0, PIECES)

    @pl.loop(0, group)
    def _(i):
        other = pl.ds(pl.multiple_of(i * local_rows, 8), local_rows)

        @pl.when(jnp.logical_or(jnp.logical_not(holds), i != in_half))
        def _():
            for m in (0, 1):
                push(tokens, tok.at[2 * m, other], fan_send.at[m, 0], fan_recv.at[m, i], (row, col, z)).wait_recv()

    def p_copy(i):
        to = (row, lax.rem(col + i, cols), z)
        at = pl.ds(pl.multiple_of(col * local_rows, 8), local_rows)
        return push(prev, prev_all.at[at], p_send.at[i], p_recv.at[col], to)

    p_keep = pltpu.make_async_copy(prev, prev_all.at[pl.ds(pl.multiple_of(col * local_rows, 8), local_rows)], p_local.at[0])
    p_keep.start()

    @pl.loop(1, cols)
    def _(i):
        p_copy(i).start()

    pairs = [push(tok.at[2 * m], tok.at[2 * m + 1], tok_send.at[1 + m], tok_recv.at[1 + m], peers[1]) for m in (0, 1)]
    for copy in pairs:
        copy.start()
    w_arrive(0)
    for copy in pairs:
        copy.wait_recv()

    depth = weight.shape[0]
    total = max(n + 4, REST * -(-(4 * per_stage - PREFILL) // (REST - 1)), LATE + GAP + 1)

    @pl.loop(0, total)
    def _(t):
        @pl.when(t < n)
        def _():
            @pl.when(t >= RING)
            def _():
                sent(t - RING)
            for copy in w_loads(t):
                copy.wait()
            slot, ws = lax.rem(t, RING), lax.rem(t, 2)

            @pl.loop(0, 2)
            def _(h):
                rows = pl.ds(pl.multiple_of(h * 4 * own, own), 4 * own)
                acc = jnp.dot(tok[0, rows], wslot[ws, pl.ds(0, depth)], preferred_element_type=jnp.float32)
                for m in (1, 2, 3):
                    acc += jnp.dot(tok[m, rows], wslot[ws, pl.ds(m * depth, depth)], preferred_element_type=jnp.float32)
                part[slot, h] = acc

            @pl.when(end)
            def _():
                @pl.loop(0, 2 * 3)
                def _(i):
                    h, g = i // 3, i % 3
                    value = part[slot, h, pl.ds(pl.multiple_of(jnp.where(low, own, 0) + g * own, own), own)]
                    code(first.at[slot, h, pl.ds(pl.multiple_of(g * own, own), own)], value)
                s1(t).start()

            @pl.when(t + AHEAD < n)
            def _():
                for m in (1, 2, 3):
                    w_copy(m, t + AHEAD).start()

            @pl.when(t + 1 < n)
            def _():
                w_arrive(t + 1)

        @pl.when(jnp.logical_not(end) & (t >= 1) & (t - 1 < n))
        def _():
            j = t - 1
            slot = lax.rem(j, RING)
            s1(j).wait_recv()

            @pl.loop(0, 2 * 2)
            def _(i):
                h, g = i // 2, i % 2
                value = part[slot, h, pl.ds(pl.multiple_of(jnp.where(low, 2 * own, 0) + g * own, own), own)]
                value += decode(r1[j, h, pl.ds(pl.multiple_of(jnp.where(low, own, 0) + g * own, own), own)])
                code(second.at[slot, h, pl.ds(pl.multiple_of(g * own, own), own)], value)
            s2(j).start()

        @pl.when(jnp.logical_not(end) & (t >= 2) & (t - 2 < n))
        def _():
            j = t - 2
            slot = lax.rem(j, RING)
            s2(j).wait_recv()
            rows = at_rows(0, 3 * own, own)
            part[slot, :, rows] = part[slot, :, rows] + decode(r2[j, :, at_rows(0, own, own)])
            s3(j).start()
            mine = part[slot, :, at_rows(own, 2 * own, own)]
            finish(j, mine + decode(r1[j, :, at_rows(0, 2 * own, own)]) + decode(r2[j, :, at_rows(own, 0, own)]))

        @pl.when(end & (t >= 4) & (t - 4 < n))
        def _():
            j = t - 4
            s3(j).wait_recv()
            finish(j, part[lax.rem(j, RING), :, at_rows(0, 3 * own, own)] + r3[j])

        turn = lax.rem(t, REST)
        p = jnp.where(turn < REST - 1, PREFILL + (REST - 1) * (t // REST) + turn, -1)
        for q in range(PIECES + 1):
            if q >= PREFILL:
                @pl.when(p == q)
                def _():
                    if q == PIECES:
                        c_landed().wait_recv()
                    g_step(0, q)
            for s in (1, 2, 3):
                @pl.when(p == s * per_stage + q)
                def _():
                    g_step(s, q)
                    if q == PIECES:
                        stage_done(s)

        @pl.when(t == 2)
        def _():
            own_copy.wait()
            block_done(z)

        @pl.when(t == LATE)
        def _():
            crossed(z)

        @pl.when(t == LATE + GAP)
        def _():
            crossed_stage(1)

    p_keep.wait()

    @pl.loop(1, cols)
    def _(i):
        source = lax.rem(col + i, cols)
        at = pl.ds(pl.multiple_of(source * local_rows, 8), local_rows)
        push(prev, prev_all.at[at], p_send.at[i], p_recv.at[source], (row, col, z)).wait_recv()
        p_copy(i).wait_send()

    crossed_stage(2)
    crossed_stage(3)

    @pl.loop(max(0, n - RING), n)
    def _(j):
        sent(j)

    @pl.loop(max(0, n - 4), n)
    def _(j):
        o_wait(j)

    @pl.loop(0, n)
    def _(j):
        o_landed(j)
        for m in (1, 2, 3):
            w_copy(m, j).wait_send()

    for way in (0, 1):
        @pl.when(sends(way))
        def _():
            for q in range(PIECES):
                g_own(way, q).wait_send()
            g_copy(way, 0, PIECES, True).wait_send()
        for s in (1, 2, 3):
            @pl.when(has(way, s) & sends(way))
            def _():
                for q in range(PIECES + 1):
                    g_copy(way, s, q, True).wait_send()
    c_copy().wait_send()
    for i in range(4):
        x_copy(i, i).wait_send()
        d_copy(row, i, i).wait_send()
        d_copy(over, i, 4 + i).wait_send()
        d_copy(near, i, i).wait_recv()
        d_copy(cross, i, 4 + i).wait_recv()

    @pl.when(jnp.logical_not(holds))
    def _():
        hop.wait_send()

    @pl.when(holds)
    def _():
        @pl.loop(1, cols)
        def _(i):
            fan(i, 0).wait_send()
            fan(i, 1).wait_send()
    for copy in pairs:
        copy.wait_send()


def product(left, right, out):
    out[...] = lax.dot_general(left[...], right[...], (((0,), (0,)), ((), ())), preferred_element_type=jnp.float32)


def local(cols, tokens, weight, prev_tokens, prev_grad):
    depth, width = weight.shape
    half = width // 2
    n = half // CC
    own = prev_grad.shape[0]
    carry = own // 2
    dma = pltpu.SemaphoreType.DMA
    anywhere = pl.BlockSpec(memory_space=pl.ANY)
    qkv, every, prev_all, _ = pl.pallas_call(
        functools.partial(kernel, n, cols, carry),
        out_shape=(
            jax.ShapeDtypeStruct((own, width), jnp.bfloat16),
            jax.ShapeDtypeStruct((16 * own, width), jnp.bfloat16),
            jax.ShapeDtypeStruct((8 * own * 2, depth), jnp.bfloat16),
            jax.ShapeDtypeStruct((n, 3, depth, CC), jnp.bfloat16),
        ),
        in_specs=[anywhere] * 4,
        out_specs=(anywhere,) * 4,
        scratch_shapes=[
            pltpu.VMEM((4, 8 * own, depth), jnp.bfloat16),
            pltpu.VMEM((2, 4 * depth, CC), jnp.bfloat16),
            pltpu.VMEM((RING, 2, 4 * own, CC), jnp.float32),
            pltpu.VMEM((RING, 2, 3 * own, CC * 3 // 2), jnp.bfloat16),
            pltpu.VMEM((RING, 2, 2 * own, CC * 3 // 2), jnp.bfloat16),
            pltpu.VMEM((n, 2, 3 * own, CC * 3 // 2), jnp.bfloat16),
            pltpu.VMEM((n, 2, 2 * own, CC * 3 // 2), jnp.bfloat16),
            pltpu.VMEM((n, 2, own, CC), jnp.float32),
            pltpu.VMEM((4, 2, own, CC), jnp.bfloat16),
            dma((1,)), dma((3,)), dma((3,)), dma((2, cols)), dma((2, cols // 2)),
            dma((3, n)), dma((3, n)), dma((2, 4)),
            dma((RING,)), dma((RING,)), dma((n,)), dma((n,)), dma((n,)),
            dma((4,)), dma((4,)), dma((n,)),
            dma((2, 4 * (PIECES + 1))), dma((2, 4 * (PIECES + 1))), dma((1,)), dma((1,)), dma((1,)), dma((4,)), dma((4,)), dma((8,)), dma((8,)),
            dma((1,)), dma((cols,)), dma((cols,)),
        ],
        compiler_params=pltpu.CompilerParams(has_side_effects=True, vmem_limit_bytes=64 * 1024 * 1024 - 65536),
        name="exchange",
    )(tokens, weight, prev_tokens, prev_grad)
    tile = math.gcd(width, 1536)
    weight_grad = pl.pallas_call(
        product,
        out_shape=jax.ShapeDtypeStruct((depth, width), jnp.float32),
        grid=(width // tile,),
        in_specs=[pl.BlockSpec((16 * own, depth), lambda i: (0, 0)), pl.BlockSpec((16 * own, tile), lambda i: (0, i))],
        out_specs=pl.BlockSpec((depth, tile), lambda i: (0, i)),
        compiler_params=pltpu.CompilerParams(vmem_limit_bytes=32 * 1024 * 1024),
        name="product",
    )(prev_all, every)
    return (qkv, weight_grad)


def solution(mesh):
    placed = (
        P("col", ("row", "depth")),
        P(("row", "depth"), "col"),
        P("col", ("row", "depth")),
        P(("row", "depth"), "col"),
    )
    cols = mesh.shape["col"]
    fits = mesh.shape["row"] == 4 and mesh.shape["depth"] == 4 and cols % 2 == 0
    return jax.shard_map(
        functools.partial(local, cols) if fits else plain,
        mesh=mesh,
        in_specs=placed,
        out_specs=(P(("row", "depth"), "col"), P(("row", "depth"), "col")),
        check_vma=False,
    )
```
